512 devices in a mesh: slab: 128 (over y, x, z_hi, core), col: 4 (over z_lo).
Axes of the slice: x: 4, y: 8, z: 8 (z_hi: 2, z_lo: 4; z = z_hi * 4 + z_lo), core: 2. Of those that a mesh axis runs over, the one named last changes fastest.
Arguments:
- volume: bfloat16 [128, 512, 6144], P('slab', 'col'), may hold values from -6 to 6
- detector_row_weight: bfloat16 [128, 512], P(None, 'col'), may hold values from -0.25 to 0.25
- tile_bank: bfloat16 [4, 128, 128], replicated, may hold values from -0.5 to 0.5
- tile_class: int32 [128], replicated, may hold values from 0 to 3
- tile_shift: int32 [128], replicated, may hold values from 0 to 47
- owner_angle: int32 [128], replicated, may hold values from 0 to 127, each once
- measured: bfloat16 [128, 128, 6144], P('slab', None, 'col'), may hold values from -6 to 6
- window_slice: int32 [128], P('slab'), may hold values from -4 to 0
- window_col: int32 [128], P('slab'), may hold values from -32 to 16
Outputs:
- projection: bfloat16 [128, 128, 6144], P('slab', None, 'col')
- correlation: float32 [128, 4, 16], P('slab')
- shifts: float32 [2, 128], P(None, 'slab')
The draws below stay inside these ranges and needn't reach their ends.
Inputs may be any that keep to these rules, and one draw needn't show every extreme that they name: `owner_angle`: every angle stands in exactly one slot.
All inputs are finite; a program needn't handle non-finite values.
Results may differ from the reference program's by a relative error of at most 0.0095.
Values may be sent and summed in bfloat16 or wider, within the bound.
No kernel may reach another device: no remote copies, remote signals or barrier semaphores. Data moves between devices by JAX's collectives and lax.ppermute only.
A program may use at most 64 MiB of HBM per device.

```python
import math
import jax
import jax.numpy as jnp
from jax import lax

NU = 6144
TILE = 128
NB = 4
RW = 512
LAG = 32
WU = 16
LAGZ = 4
WZ = 4
NT = 48
RQ = 128
NZ = 128
ANG = 128
N_COL = 4


def plant(result, rng, smallest, top_value):
    dims = result.shape
    place = [jax.random.randint(jax.random.fold_in(rng, axis), (), 0, dims[axis]) for axis in range(len(dims))]
    result = result.at[tuple(place)].set(smallest)
    longest = dims.index(max(dims))
    place[longest] = (place[longest] + 1) % dims[longest]
    return result.at[tuple(place)].set(top_value)


def block_levels(stream_key, shape, split, least, top_value):
    gain, own = 1.0, jax.random.fold_in(stream_key, 6)
    for position, parts in split:
        draws = jnp.exp(jax.random.uniform(jax.random.fold_in(own, position), (parts,), jnp.float32, least / len(split), top_value / len(split)))
        gain = gain * jnp.repeat(draws, shape[position] // parts).reshape([-1 if axis == position else 1 for axis in range(len(shape))])
    return gain


def scatter_about(key, extent, scale, most, pieces=(), held_as=jnp.bfloat16):
    drawn = jax.random.normal(key, extent, jnp.float32) * scale
    if len(pieces) > 0:
        drawn = block_levels(key, extent, pieces, -0.22, 0.18) * drawn
    return jnp.clip(drawn, min=-most, max=most).astype(held_as)


def setup_inputs(seed: int = 0) -> dict:
    streams_of = jax.random.split(jax.random.key(seed), 10)
    return {
        "volume": scatter_about(streams_of[0], (NZ, RW, NU), 1.0, 6.0, ((0, 128), (1, 4))),
        "detector_row_weight": scatter_about(streams_of[1], (ANG, RW), RW ** -0.5, 0.25, ((1, 4),)),
        "tile_bank": scatter_about(streams_of[2], (NB, TILE, TILE), TILE ** -0.5, 0.5),
        "tile_class": plant(jax.random.randint(streams_of[3], (ANG,), 0, NB), jax.random.fold_in(streams_of[3], 1), 0, NB - 1).astype(jnp.int32),
        "tile_shift": plant(jax.random.randint(streams_of[4], (ANG,), 0, NT), jax.random.fold_in(streams_of[4], 1), 0, NT - 1).astype(jnp.int32),
        "owner_angle": jax.random.permutation(streams_of[5], ANG).astype(jnp.int32),
        "measured": scatter_about(streams_of[6], (ANG, NZ, NU), 1.0, 6.0, ((0, 128), (2, 4))),
        "window_slice": plant(jax.random.randint(streams_of[7], (ANG,), 0 - LAGZ, LAGZ - WZ + 1), jax.random.fold_in(streams_of[7], 1), 0 - LAGZ, LAGZ - WZ).astype(jnp.int32),
        "window_col": plant(jax.random.randint(streams_of[8], (ANG,), 0 - LAG, LAG - WU + 1), jax.random.fold_in(streams_of[8], 1), 0 - LAG, LAG - WU).astype(jnp.int32),
    }


def reference(volume, detector_row_weight, tile_bank, tile_class, tile_shift, owner_angle, measured, window_slice, window_col):
    chosen = jnp.take(detector_row_weight, owner_angle, axis=0).astype(jnp.float32)
    shift_chosen = jnp.take(tile_shift, owner_angle)
    system_operators = jnp.take(tile_bank, jnp.take(tile_class, owner_angle), axis=0).astype(jnp.float32)
    targets = jnp.arange(NT, dtype=jnp.int32)
    sources = ((targets[None, :] - shift_chosen[:, None]) % NT).astype(jnp.int32)

    def project_plane(plane):
        plane_wide = plane.astype(jnp.float32)
        summed = jnp.zeros((ANG, NU), jnp.float32)
        for block_index in range(N_COL):
            lower = block_index * RQ
            ray_sums = jnp.dot(chosen[:, lower:lower + RQ], plane_wide[lower:lower + RQ], precision=lax.Precision.HIGHEST, preferred_element_type=jnp.float32).astype(jnp.bfloat16)
            rolled = jnp.take_along_axis(ray_sums.reshape(ANG, NT, TILE), sources[:, :, None], axis=1)
            spread = jnp.einsum('ktc,kcd->ktd', rolled.astype(jnp.float32), system_operators, precision=lax.Precision.HIGHEST).astype(jnp.bfloat16)
            summed = summed + spread.reshape(ANG, NU).astype(jnp.float32)
        return summed.astype(jnp.bfloat16)
    planes = lax.map(project_plane, volume)
    projection = jnp.transpose(planes, (1, 0, 2))
    norm_factor = 1.0 / math.sqrt(NZ * NU)
    lag_slices = jnp.arange(WZ, dtype=jnp.int32)
    lag_columns = jnp.arange(WU, dtype=jnp.int32)

    def correlate_slot(item):
        proj_slot, observed_slot_data, start_slice, start_col = item
        forward_spectrum = jnp.fft.fft2(proj_slot.astype(jnp.float32))
        observed_spectrum = jnp.fft.fft2(observed_slot_data.astype(jnp.float32))
        periodic_wrap = jnp.real(jnp.fft.ifft2(jnp.conj(forward_spectrum) * observed_spectrum))
        slice_rows = ((start_slice + lag_slices) % NZ).astype(jnp.int32)
        column_rows = ((start_col + lag_columns) % NU).astype(jnp.int32)
        return jnp.take(jnp.take(periodic_wrap, slice_rows, axis=0), column_rows, axis=1) * norm_factor
    correlation = lax.map(correlate_slot, (projection, measured, window_slice, window_col))
    weight_grid = correlation * correlation
    along_slices = (window_slice[:, None] + lag_slices[None, :]).astype(jnp.float32) / LAGZ
    along_columns = (window_col[:, None] + lag_columns[None, :]).astype(jnp.float32) / LAG
    denominator = lax.optimization_barrier(jnp.mean(weight_grid, axis=(1, 2))) + 1e-06
    shift_slices = lax.optimization_barrier(jnp.mean(weight_grid * along_slices[:, :, None], axis=(1, 2))) / denominator
    shift_columns = lax.optimization_barrier(jnp.mean(weight_grid * along_columns[:, None, :], axis=(1, 2))) / denominator
    return (projection, correlation, jnp.stack([shift_slices, shift_columns]))
```

```python
import math

import jax
import jax.numpy as jnp
from jax import lax
from jax.experimental import pallas as pl
from jax.experimental.pallas import tpu as pltpu
from jax.sharding import PartitionSpec as P

LAG = 32
WU = 16
LAGZ = 4
WZ = 4
ROWS = 144


def project_kernel(place, owner, shift, cls, weights, bank, volume, *outs_held):
    outs, held = outs_held[:-1], outs_held[-1]
    angles = weights.shape[0]
    columns = volume.shape[1]
    tile = bank.shape[1]
    banks = bank.shape[0]
    tiles = columns // tile
    quarters = len(outs)
    per = tiles // quarters
    lane = lax.broadcasted_iota(jnp.int32, (angles, angles), 1)
    wide = jnp.broadcast_to(owner[...].astype(jnp.float32), (angles, angles))
    picks = wide.T.astype(jnp.int32) == lane
    onehot = picks.astype(jnp.float32)
    shifts = jnp.sum(onehot * shift[...].astype(jnp.float32), axis=1, keepdims=True)
    classes = jnp.sum(onehot * cls[...].astype(jnp.float32), axis=1, keepdims=True)
    shifts = shifts.astype(jnp.int32) + (tiles - per * place[0])
    shifts = jnp.where(shifts >= tiles, shifts - tiles, shifts)
    chosen = jnp.dot(
        onehot.astype(jnp.bfloat16), weights[...], preferred_element_type=jnp.float32
    ).astype(jnp.bfloat16)
    classes = jnp.broadcast_to(classes, (angles, tile)).astype(jnp.int32)
    masks = [(classes == c).astype(jnp.bfloat16) for c in range(banks)]
    stacked = bank[...].reshape(banks * tile, tile)
    width = 4 * tile
    for j in range(columns // width):
        ray = jnp.dot(
            chosen, volume[:, j * width : (j + 1) * width], preferred_element_type=jnp.float32
        ).astype(jnp.bfloat16)
        for t in range(width // tile):
            piece = ray[:, t * tile : (t + 1) * tile]
            spreadable = jnp.concatenate([piece * m for m in masks], axis=1)
            at = j * width + t * tile
            held[:, at : at + tile] = jnp.dot(
                spreadable, stacked, preferred_element_type=jnp.float32
            )
    group = 8
    bits = (tiles - 1).bit_length()
    for g in range(angles // group):
        rows = slice(g * group, (g + 1) * group)
        amount = jnp.broadcast_to(shifts[rows], (group, tile))
        parts = [held[rows, t * tile : (t + 1) * tile] for t in range(tiles)]
        for b in range(bits):
            keep = ((amount >> b) & 1) == 0
            parts = [
                jnp.where(keep, parts[t], parts[(t - (1 << b)) % tiles]) for t in range(tiles)
            ]
        for t in range(tiles):
            q, c = divmod(t, per)
            outs[q][rows, c * tile : (c + 1) * tile] = parts[t].astype(jnp.bfloat16)


def project(place, owner, shift, cls, weights, bank, volume, quarters):
    angles = weights.shape[0]
    columns = volume.shape[1]
    return pl.pallas_call(
        project_kernel,
        out_shape=[jax.ShapeDtypeStruct((angles, columns // quarters), jnp.bfloat16)] * quarters,
        in_specs=[pl.BlockSpec(memory_space=pltpu.SMEM)]
        + [pl.BlockSpec(memory_space=pltpu.VMEM)] * 6,
        scratch_shapes=[pltpu.VMEM((angles, columns), jnp.float32)],
        name="project",
    )(place, owner[None], shift[None], cls[None], weights, bank, volume)


def correlate_kernel(starts, owned, across, out):
    slices, columns = owned.shape
    tile = 128
    tiles = columns // tile
    start_slice = starts[0]
    first = starts[1] + LAG
    pieces = []
    for a in range(WZ):
        turn = lax.rem(2 * slices - start_slice - a, slices)
        row = []
        for t in range(tiles):
            block = across[pl.ds(first + t * tile, ROWS), :]
            row.append(pltpu.roll(block, turn, 1).astype(jnp.bfloat16))
        pieces.append(jnp.concatenate(row, axis=1))
    lhs = jnp.concatenate(pieces, axis=0)
    rhs = jnp.concatenate(
        [owned[:, t * tile : (t + 1) * tile] for t in range(tiles)], axis=0
    )
    sums = jnp.dot(lhs, rhs, preferred_element_type=jnp.float32)
    lanes = lax.broadcasted_iota(jnp.int32, (8, tile), 1)
    subs = lax.broadcasted_iota(jnp.int32, (8, tile), 0)
    results = []
    for a in range(WZ):
        total = jnp.zeros((8, tile), jnp.float32)
        for i in range(ROWS // 8):
            block = sums[a * ROWS + i * 8 : a * ROWS + i * 8 + 8]
            if i < WU // 8:
                block = jnp.where(lanes < tile // 2, block, 0.0)
            if i >= tile // 8:
                block = jnp.where(lanes >= tile // 2, block, 0.0)
            total = total + pltpu.roll(block, (-8 * i) % tile, 1)
        aligned = jnp.zeros((8, tile), jnp.float32)
        for d in range(WU):
            here = ((subs - d) & (tile - 1)) == lanes
            value = jnp.sum(jnp.where(here, total, 0.0))
            aligned = jnp.where(lanes == d, value, aligned)
        results.append(aligned[0:1])
    results.append(jnp.zeros((8 - WZ, tile), jnp.float32))
    out[...] = jnp.concatenate(results, axis=0)


def correlate(starts, owned, across):
    return pl.pallas_call(
        correlate_kernel,
        out_shape=jax.ShapeDtypeStruct((8, 128), jnp.float32),
        in_specs=[
            pl.BlockSpec(memory_space=pltpu.SMEM),
            pl.BlockSpec(memory_space=pltpu.VMEM),
            pl.BlockSpec(memory_space=pltpu.VMEM),
        ],
        name="correlate",
    )(starts, owned, across)


def local(
    volume,
    detector_row_weight,
    tile_bank,
    tile_class,
    tile_shift,
    owner_angle,
    measured,
    window_slice,
    window_col,
):
    count = lax.axis_size("col")
    place = lax.axis_index("col").astype(jnp.int32)[None]
    ring = [[(i, (i + d) % count) for i in range(count)] for d in range(count)]
    pieces = project(
        place, owner_angle, tile_shift, tile_class, detector_row_weight, tile_bank, volume[0], count
    )
    total = pieces[0].astype(jnp.float32)
    for d in range(1, count):
        total = total + lax.ppermute(pieces[d], "col", ring[d]).astype(jnp.float32)
    summed = total.astype(jnp.bfloat16)[:, None, :]
    owned = lax.all_to_all(summed, "slab", split_axis=0, concat_axis=1, tiled=True)
    seen = measured[0]
    slices, quarter = seen.shape
    low = lax.ppermute(seen[:, quarter - LAG :], "col", ring[1])
    high = lax.ppermute(seen[:, :LAG], "col", ring[count - 1])
    rest = jnp.zeros((128 - 2 * LAG, slices), jnp.bfloat16)
    across = jnp.concatenate([low.T, seen.T, high.T, rest], axis=0).astype(jnp.float32)
    starts = jnp.concatenate([window_slice, window_col])
    part = correlate(starts, owned[0], across)[None, :WZ, :WU]
    norm_factor = 1.0 / math.sqrt(slices * quarter * count)
    totals = lax.psum(part * norm_factor, "col")
    lag_slices = jnp.arange(WZ, dtype=jnp.int32)
    lag_columns = jnp.arange(WU, dtype=jnp.int32)
    weight_grid = totals * totals
    along_slices = (window_slice[:, None] + lag_slices[None, :]).astype(jnp.float32) / LAGZ
    along_columns = (window_col[:, None] + lag_columns[None, :]).astype(jnp.float32) / LAG
    denominator = jnp.mean(weight_grid, axis=(1, 2)) + 1e-06
    shift_slices = jnp.mean(weight_grid * along_slices[:, :, None], axis=(1, 2)) / denominator
    shift_columns = jnp.mean(weight_grid * along_columns[:, None, :], axis=(1, 2)) / denominator
    return (owned, totals, jnp.stack([shift_slices, shift_columns]))


def solution(mesh):
    return jax.shard_map(
        local,
        mesh=mesh,
        in_specs=(
            P("slab", "col", None),
            P(None, "col"),
            P(),
            P(),
            P(),
            P(),
            P("slab", None, "col"),
            P("slab"),
            P("slab"),
        ),
        out_specs=(P("slab", None, "col"), P("slab", None, None), P(None, "slab")),
        check_vma=False,
    )
```

```python
import math

import jax
import jax.numpy as jnp
from jax import lax
from jax.experimental import pallas as pl
from jax.experimental.pallas import tpu as pltpu
from jax.sharding import PartitionSpec as P

LAG = 32
WU = 16
LAGZ = 4
WZ = 4
ROWS = 144


def project_kernel(owner, shift, cls, weights, bank, volume, out, held):
    angles = weights.shape[0]
    columns = volume.shape[1]
    tile = bank.shape[1]
    banks = bank.shape[0]
    tiles = columns // tile
    planes = out.shape[1]
    kinds = angles // planes
    quarters = out.shape[0] // kinds
    per = tiles // quarters
    lane = lax.broadcasted_iota(jnp.int32, (angles, angles), 1)
    row = lax.broadcasted_iota(jnp.int32, (angles, angles), 0)
    order = ((row % planes) * kinds + row // planes == lane).astype(jnp.bfloat16)
    wide = jnp.broadcast_to(owner[...].astype(jnp.float32), (angles, angles))
    picks = (wide.T.astype(jnp.int32) == lane).astype(jnp.bfloat16)
    onehot = jnp.dot(order, picks, preferred_element_type=jnp.float32)
    shifts = jnp.sum(onehot * shift[...].astype(jnp.float32), axis=1, keepdims=True)
    classes = jnp.sum(onehot * cls[...].astype(jnp.float32), axis=1, keepdims=True)
    shifts = shifts.astype(jnp.int32)
    chosen = jnp.dot(
        onehot.astype(jnp.bfloat16), weights[...], preferred_element_type=jnp.float32
    ).astype(jnp.bfloat16)
    classes = jnp.broadcast_to(classes, (angles, tile)).astype(jnp.int32)
    masks = [(classes == c).astype(jnp.bfloat16) for c in range(banks)]
    stacked = bank[...].reshape(banks * tile, tile)
    width = 4 * tile
    for j in range(columns // width):
        ray = jnp.dot(
            chosen, volume[:, j * width : (j + 1) * width], preferred_element_type=jnp.float32
        ).astype(jnp.bfloat16)
        for t in range(width // tile):
            piece = ray[:, t * tile : (t + 1) * tile]
            spreadable = jnp.concatenate([piece * m for m in masks], axis=1)
            at = j * width + t * tile
            held[:, at : at + tile] = jnp.dot(
                spreadable, stacked, preferred_element_type=jnp.float32
            )
    group = 8
    bits = (tiles - 1).bit_length()
    for g in range(angles // group):
        rows = slice(g * group, (g + 1) * group)
        amount = jnp.broadcast_to(shifts[rows], (group, tile))
        parts = [held[rows, t * tile : (t + 1) * tile] for t in range(tiles)]
        for b in range(bits):
            keep = ((amount >> b) & 1) == 0
            parts = [
                jnp.where(keep, parts[t], parts[(t - (1 << b)) % tiles]) for t in range(tiles)
            ]
        kind, plane = divmod(g * group, planes)
        high, low = divmod(kind, 2)
        for t in range(tiles):
            q, c = divmod(t, per)
            out[(high * quarters + q) * 2 + low, plane : plane + group, c * tile : (c + 1) * tile] = (
                parts[t].astype(jnp.bfloat16)
            )


def project(owner, shift, cls, weights, bank, volume, quarters, kinds):
    angles = weights.shape[0]
    columns = volume.shape[1]
    return pl.pallas_call(
        project_kernel,
        out_shape=jax.ShapeDtypeStruct(
            (quarters * kinds, angles // kinds, columns // quarters), jnp.bfloat16
        ),
        scratch_shapes=[pltpu.VMEM((angles, columns), jnp.float32)],
        name="project",
    )(owner[None], shift[None], cls[None], weights, bank, volume)


def correlate_kernel(starts, owned, across, out):
    slices, columns = owned.shape
    tile = 128
    tiles = columns // tile
    start_slice = starts[0]
    first = starts[1] + LAG
    pieces = []
    for a in range(WZ):
        turn = lax.rem(2 * slices - start_slice - a, slices)
        row = []
        for t in range(tiles):
            block = across[pl.ds(first + t * tile, ROWS), :]
            row.append(pltpu.roll(block, turn, 1).astype(jnp.bfloat16))
        pieces.append(jnp.concatenate(row, axis=1))
    lhs = jnp.concatenate(pieces, axis=0)
    rhs = jnp.concatenate(
        [owned[:, t * tile : (t + 1) * tile] for t in range(tiles)], axis=0
    )
    sums = jnp.dot(lhs, rhs, preferred_element_type=jnp.float32)
    lanes = lax.broadcasted_iota(jnp.int32, (8, tile), 1)
    subs = lax.broadcasted_iota(jnp.int32, (8, tile), 0)
    results = []
    for a in range(WZ):
        total = jnp.zeros((8, tile), jnp.float32)
        for i in range(ROWS // 8):
            block = sums[a * ROWS + i * 8 : a * ROWS + i * 8 + 8]
            if i < WU // 8:
                block = jnp.where(lanes < tile // 2, block, 0.0)
            if i >= tile // 8:
                block = jnp.where(lanes >= tile // 2, block, 0.0)
            total = total + pltpu.roll(block, (-8 * i) % tile, 1)
        aligned = jnp.zeros((8, tile), jnp.float32)
        for d in range(WU):
            here = ((subs - d) & (tile - 1)) == lanes
            value = jnp.sum(jnp.where(here, total, 0.0))
            aligned = jnp.where(lanes == d, value, aligned)
        results.append(aligned[0:1])
    results.append(jnp.zeros((8 - WZ, tile), jnp.float32))
    out[...] = jnp.concatenate(results, axis=0)


def correlate(starts, owned, across):
    return pl.pallas_call(
        correlate_kernel,
        out_shape=jax.ShapeDtypeStruct((8, 128), jnp.float32),
        in_specs=[
            pl.BlockSpec(memory_space=pltpu.SMEM),
            pl.BlockSpec(memory_space=pltpu.VMEM),
            pl.BlockSpec(memory_space=pltpu.VMEM),
        ],
        name="correlate",
    )(starts, owned, across)


def local(
    volume,
    detector_row_weight,
    tile_bank,
    tile_class,
    tile_shift,
    owner_angle,
    measured,
    window_slice,
    window_col,
):
    count = lax.axis_size("zl")
    halves = lax.axis_size("zh")
    cores = lax.axis_size("co")
    kinds = halves * cores
    ring = [[(i, (i + d) % count) for i in range(count)] for d in range(count)]
    pieces = project(
        owner_angle, tile_shift, tile_class, detector_row_weight, tile_bank, volume[0], count, kinds
    )
    parts = lax.all_to_all(pieces, ("zh", "zl", "co"), 0, 0, tiled=True)
    planes, quarter = parts.shape[1:]
    parts = parts.reshape(halves, count, cores, planes, quarter)
    summed = jnp.sum(parts.astype(jnp.float32), axis=1).astype(jnp.bfloat16)
    summed = jnp.transpose(summed.reshape(kinds, planes, quarter), (1, 0, 2))
    owned = lax.all_to_all(summed, ("y", "x"), 0, 0, tiled=True)
    owned = owned.reshape(1, planes * kinds, quarter)
    seen = measured[0]
    slices, quarter = seen.shape
    low = lax.ppermute(seen[:, quarter - LAG :], "zl", ring[1])
    high = lax.ppermute(seen[:, :LAG], "zl", ring[count - 1])
    rest = jnp.zeros((128 - 2 * LAG, slices), jnp.bfloat16)
    across = jnp.concatenate([low.T, seen.T, high.T, rest], axis=0).astype(jnp.float32)
    starts = jnp.concatenate([window_slice, window_col])
    part = correlate(starts, owned[0], across)[None, :WZ, :WU]
    norm_factor = 1.0 / math.sqrt(slices * quarter * count)
    totals = lax.psum(part * norm_factor, "zl")
    lag_slices = jnp.arange(WZ, dtype=jnp.int32)
    lag_columns = jnp.arange(WU, dtype=jnp.int32)
    weight_grid = totals * totals
    along_slices = (window_slice[:, None] + lag_slices[None, :]).astype(jnp.float32) / LAGZ
    along_columns = (window_col[:, None] + lag_columns[None, :]).astype(jnp.float32) / LAG
    denominator = jnp.mean(weight_grid, axis=(1, 2)) + 1e-06
    shift_slices = jnp.mean(weight_grid * along_slices[:, :, None], axis=(1, 2)) / denominator
    shift_columns = jnp.mean(weight_grid * along_columns[:, None, :], axis=(1, 2)) / denominator
    return (owned, totals, jnp.stack([shift_slices, shift_columns]))


def solution(mesh):
    slab, col = mesh.axis_names
    cols = mesh.shape[col]
    rows = mesh.shape[slab]
    parts = jax.sharding.Mesh(
        mesh.devices.reshape(rows // 16, 4, 2, 2, cols), ("y", "x", "zh", "co", "zl")
    )
    slab = ("y", "x", "zh", "co")
    return jax.shard_map(
        local,
        mesh=parts,
        in_specs=(
            P(slab, "zl", None),
            P(None, "zl"),
            P(),
            P(),
            P(),
            P(),
            P(slab, None, "zl"),
            P(slab),
            P(slab),
        ),
        out_specs=(P(slab, None, "zl"), P(slab, None, None), P(None, slab)),
        check_vma=False,
    )
```

```python
import functools
import math

import jax
import jax.numpy as jnp
from jax import lax
from jax.experimental import pallas as pl
from jax.experimental.pallas import tpu as pltpu
from jax.sharding import PartitionSpec as P

LAG = 32
WU = 16
LAGZ = 4
WZ = 4
ROWS = 144
STEPS = (0, 1, -1, 2, -2, 3, -3)


def project_kernel(place, *refs):
    sources, outs, rest = refs[:6], refs[6:-9], refs[-9:]
    owner, shift, cls, weights, bank, volume, held, ready, sems = rest
    angles = weights.shape[0]
    chunks, _, width = volume.shape
    columns = chunks * width
    tile = bank.shape[1]
    banks = bank.shape[0]
    tiles = columns // tile
    peers, planes = ready.shape[:2]
    halves = angles // planes
    quarters = peers // halves
    per = tiles // quarters
    small = [
        pltpu.make_async_copy(source, target, sems.at[i])
        for i, (source, target) in enumerate(zip(sources[:5], rest[:5]))
    ]
    large = [
        pltpu.make_async_copy(
            sources[5].at[:, j * width : (j + 1) * width], volume.at[j], sems.at[5 + j]
        )
        for j in range(chunks)
    ]
    for copy in small + large:
        copy.start()
    for copy in small:
        copy.wait()
    lane = lax.broadcasted_iota(jnp.int32, (angles, angles), 1)
    row = lax.broadcasted_iota(jnp.int32, (angles, angles), 0)
    slot = row % planes
    order = (slot // 2 * 4 + row // planes * 2 + slot % 2 == lane).astype(jnp.bfloat16)
    wide = jnp.broadcast_to(owner[...].astype(jnp.float32), (angles, angles))
    picks = (wide.T.astype(jnp.int32) == lane).astype(jnp.bfloat16)
    onehot = jnp.dot(order, picks, preferred_element_type=jnp.float32)
    shifts = jnp.sum(onehot * shift[...].astype(jnp.float32), axis=1, keepdims=True)
    classes = jnp.sum(onehot * cls[...].astype(jnp.float32), axis=1, keepdims=True)
    shifts = shifts.astype(jnp.int32)
    chosen = jnp.dot(
        onehot.astype(jnp.bfloat16), weights[...], preferred_element_type=jnp.float32
    ).astype(jnp.bfloat16)
    classes = jnp.broadcast_to(classes, (angles, tile)).astype(jnp.int32)
    masks = [(classes == c).astype(jnp.bfloat16) for c in range(banks)]
    stacked = bank[...].reshape(banks * tile, tile)
    for j in range(chunks):
        large[j].wait()
        ray = jnp.dot(chosen, volume[j], preferred_element_type=jnp.float32).astype(jnp.bfloat16)
        for t in range(width // tile):
            piece = ray[:, t * tile : (t + 1) * tile]
            spreadable = jnp.concatenate([piece * m for m in masks], axis=1)
            at = j * width + t * tile
            held[:, at : at + tile] = jnp.dot(
                spreadable, stacked, preferred_element_type=jnp.float32
            )
    group = 8
    bits = (tiles - 1).bit_length()
    for g in range(angles // group):
        rows = slice(g * group, (g + 1) * group)
        amount = jnp.broadcast_to(shifts[rows], (group, tile))
        parts = [held[rows, t * tile : (t + 1) * tile] for t in range(tiles)]
        for b in range(bits):
            keep = ((amount >> b) & 1) == 0
            parts = [
                jnp.where(keep, parts[t], parts[(t - (1 << b)) % tiles]) for t in range(tiles)
            ]
        high, plane = divmod(g * group, planes)
        for t in range(tiles):
            q, c = divmod(t, per)
            ready[high * quarters + q, plane : plane + group, c * tile : (c + 1) * tile] = parts[
                t
            ].astype(jnp.bfloat16)
    for d in range(peers):
        outs[d][...] = ready[(place[0] + d) & (peers - 1)]


def project(place, owner, shift, cls, weights, bank, volume, quarters, halves):
    angles = weights.shape[0]
    columns = volume.shape[1]
    peers = quarters * halves
    block = (angles // halves, columns // quarters)
    chunks = 8
    small = (owner[None], shift[None], cls[None], weights, bank)
    return pl.pallas_call(
        project_kernel,
        out_shape=[jax.ShapeDtypeStruct(block, jnp.bfloat16)] * peers,
        in_specs=[pl.BlockSpec(memory_space=pltpu.SMEM)]
        + [pl.BlockSpec(memory_space=pltpu.HBM)] * 6,
        out_specs=[pl.BlockSpec(memory_space=pltpu.VMEM)] * peers,
        scratch_shapes=[pltpu.VMEM(x.shape, x.dtype) for x in small]
        + [
            pltpu.VMEM((chunks, volume.shape[0], columns // chunks), volume.dtype),
            pltpu.VMEM((angles, columns), jnp.float32),
            pltpu.VMEM((peers,) + block, jnp.bfloat16),
            pltpu.SemaphoreType.DMA((len(small) + chunks,)),
        ],
        name="project",
    )(place, *small, volume)


def collect_kernel(place, *refs):
    terms, (out, held) = refs[:-2], refs[-2:]
    quarters = 4
    half = place[0] // quarters
    col = place[0] % quarters
    rows, columns = terms[0].shape
    strips = out.shape[1] // 2
    width = out.shape[2]
    low = high = None
    for ref, d in zip(terms, STEPS):
        same = (col - d >= 0) & (col - d < quarters)
        first = jnp.where(same, half, 1 - half) == 0
        weight = jnp.where(first, 1.0, 0.0)
        value = ref[...].astype(jnp.float32)
        low = value * weight if low is None else low + value * weight
        high = value * (1.0 - weight) if high is None else high + value * (1.0 - weight)
    count = 2 * rows * strips
    tile = held.shape[1]
    for h, total in enumerate((low, high)):
        for p in range(strips):
            for t in range(width // tile):
                at = p * width + t * tile
                held[pl.ds(t * count + h * strips + p, rows, stride=2 * strips), :] = total[
                    :, at : at + tile
                ]
    for t in range(width // tile):
        block = held[t * count : (t + 1) * count].astype(jnp.bfloat16)
        out[:, :, t * tile : (t + 1) * tile] = block.reshape(rows, 2 * strips, tile)


def collect(place, terms):
    rows, columns = terms[0].shape
    strips = 4
    shape = (rows, 2 * strips, columns // strips)
    return pl.pallas_call(
        collect_kernel,
        out_shape=jax.ShapeDtypeStruct(shape, jnp.bfloat16),
        in_specs=[pl.BlockSpec(memory_space=pltpu.SMEM)]
        + [pl.BlockSpec(memory_space=pltpu.VMEM)] * len(terms),
        scratch_shapes=[pltpu.VMEM((2 * rows * columns // 128, 128), jnp.float32)],
        compiler_params=pltpu.CompilerParams(vmem_limit_bytes=8 * 2**20),
        name="collect",
    )(place, *terms)


def correlate_kernel(norm, starts, parts, across, owned, out, mixed, sorted_rows, wide):
    blocks, per_block, width = parts.shape
    strips = per_block // 2
    slices, columns = owned.shape
    tile = 128
    tiles = columns // tile
    count = blocks * per_block
    for t in range(width // tile):
        block = parts[:, :, t * tile : (t + 1) * tile].astype(jnp.float32)
        mixed[t * count : (t + 1) * count] = block.reshape(count, tile)
    for core in range(2):
        for high in range(2):
            for p in range(strips):
                for t in range(width // tile):
                    at = (p * width // tile + t) * slices
                    sorted_rows[pl.ds(at + high * 2 + core, blocks // 2, stride=4), :] = mixed[
                        pl.ds(
                            t * count + (core * 2 + high) * strips + p,
                            blocks // 2,
                            stride=2 * per_block,
                        ),
                        :,
                    ]
    rhs = sorted_rows[...].astype(jnp.bfloat16)
    for t in range(tiles):
        owned[:, t * tile : (t + 1) * tile] = rhs[t * slices : (t + 1) * slices]
    wide[...] = across[...].astype(jnp.float32)
    start_slice = starts[0]
    first = starts[1] + LAG
    pieces = []
    for a in range(WZ):
        turn = lax.rem(2 * slices - start_slice - a, slices)
        row = []
        for t in range(tiles):
            block = wide[pl.ds(first + t * tile, ROWS), :]
            row.append(pltpu.roll(block, turn, 1).astype(jnp.bfloat16))
        pieces.append(jnp.concatenate(row, axis=1))
    lhs = jnp.concatenate(pieces, axis=0)
    sums = jnp.dot(lhs, rhs, preferred_element_type=jnp.float32)
    lanes = lax.broadcasted_iota(jnp.int32, (8, tile), 1)
    subs = lax.broadcasted_iota(jnp.int32, (8, tile), 0)
    results = []
    for a in range(WZ):
        total = jnp.zeros((8, tile), jnp.float32)
        for i in range(ROWS // 8):
            block = sums[a * ROWS + i * 8 : a * ROWS + i * 8 + 8]
            if i < WU // 8:
                block = jnp.where(lanes < tile // 2, block, 0.0)
            if i >= tile // 8:
                block = jnp.where(lanes >= tile // 2, block, 0.0)
            total = total + pltpu.roll(block, (-8 * i) % tile, 1)
        aligned = jnp.zeros((8, tile), jnp.float32)
        for d in range(WU):
            here = ((subs - d) & (tile - 1)) == lanes
            value = jnp.sum(jnp.where(here, total, 0.0))
            aligned = jnp.where(lanes == d, value, aligned)
        results.append(aligned[0:1])
    results.append(jnp.zeros((8 - WZ, tile), jnp.float32))
    out[...] = jnp.concatenate(results, axis=0) * norm


def correlate(norm, starts, parts, across):
    blocks, per_block, width = parts.shape
    strips = per_block // 2
    slices, columns = blocks * 2, strips * width
    vmem = pl.BlockSpec(memory_space=pltpu.VMEM)
    return pl.pallas_call(
        functools.partial(correlate_kernel, norm),
        out_shape=[
            jax.ShapeDtypeStruct((slices, columns), jnp.bfloat16),
            jax.ShapeDtypeStruct((8, 128), jnp.float32),
        ],
        in_specs=[pl.BlockSpec(memory_space=pltpu.SMEM), vmem, vmem],
        scratch_shapes=[
            pltpu.VMEM((slices * columns // 128, 128), jnp.float32),
            pltpu.VMEM((slices * columns // 128, 128), jnp.float32),
            pltpu.VMEM(across.shape, jnp.float32),
        ],
        compiler_params=pltpu.CompilerParams(vmem_limit_bytes=14 * 2**20),
        name="correlate",
    )(starts, parts, across)


def finish_kernel(starts, totals, correlation, shifts):
    values = totals[0:WZ, 0:WU]
    correlation[0] = values
    weights = values * values
    lag_slice = starts[0] + lax.broadcasted_iota(jnp.int32, (WZ, WU), 0)
    lag_col = starts[1] + lax.broadcasted_iota(jnp.int32, (WZ, WU), 1)
    count = WZ * WU

    def mean(x):
        return jnp.sum(jnp.sum(x, axis=1, keepdims=True), axis=0, keepdims=True) / count

    denominator = mean(weights) + 1e-06
    by_slice = mean(weights * (lag_slice.astype(jnp.float32) / LAGZ)) / denominator
    by_col = mean(weights * (lag_col.astype(jnp.float32) / LAG)) / denominator
    shifts[...] = jnp.concatenate([by_slice, by_col], axis=1)


def finish(starts, totals):
    return pl.pallas_call(
        finish_kernel,
        out_shape=[
            jax.ShapeDtypeStruct((1, WZ, WU), jnp.float32),
            jax.ShapeDtypeStruct((1, 2), jnp.float32),
        ],
        in_specs=[
            pl.BlockSpec(memory_space=pltpu.SMEM),
            pl.BlockSpec(memory_space=pltpu.VMEM),
        ],
        compiler_params=pltpu.CompilerParams(vmem_limit_bytes=2 * 2**20),
        name="finish",
    )(starts, totals)


def local(
    volume,
    detector_row_weight,
    tile_bank,
    tile_class,
    tile_shift,
    owner_angle,
    measured,
    window_slice,
    window_col,
):
    count = lax.axis_size("zl")
    halves = lax.axis_size("zh")
    peers = count * halves
    line = ("zh", "zl")
    place = lax.axis_index(line).astype(jnp.int32)[None]

    def hop(value, d, keep=None):
        pairs = [(i, (i + d) % peers) for i in range(peers) if keep is None or i % count in keep]
        return lax.ppermute(value, line, pairs)

    items = project(
        place, owner_angle, tile_shift, tile_class, detector_row_weight, tile_bank, volume[0],
        count, halves,
    )
    ahead = hop(items[4], 1, (0, 1))
    behind = hop(items[4], peers - 1, (2, 3))
    got = {d: hop(items[d % peers], d % peers) for d in (2, -2, 1, -1)}
    got[3] = hop(items[3] + ahead, 3)
    got[-3] = hop(items[5] + behind, 5)
    got[0] = items[0]
    packed = collect(place, [got[d] for d in STEPS])
    parts = lax.all_to_all(packed, ("y", "x", "co"), 0, 0, tiled=True)
    seen, _ = lax.optimization_barrier((measured[0], packed))
    slices, quarter = seen.shape
    ring = [(i, (i + 1) % count) for i in range(count)]
    back = [(target, source) for source, target in ring]
    low = lax.ppermute(seen[:, quarter - LAG :], "zl", ring)
    high = lax.ppermute(seen[:, :LAG], "zl", back)
    rest = jnp.zeros((128 - 2 * LAG, slices), jnp.bfloat16)
    across = jnp.concatenate([low.T, seen.T, high.T, rest], axis=0)
    starts = jnp.concatenate([window_slice, window_col])
    norm_factor = 1.0 / math.sqrt(slices * quarter * count)
    owned, part = correlate(norm_factor, starts, parts, across)
    totals, shifts = finish(starts, lax.psum(part, "zl"))
    return (owned[None], totals, shifts.T)


def solution(mesh):
    slab, col = mesh.axis_names
    cols = mesh.shape[col]
    rows = mesh.shape[slab]
    parts = jax.sharding.Mesh(
        mesh.devices.reshape(rows // 16, 4, 2, 2, cols), ("y", "x", "zh", "co", "zl")
    )
    slab = ("y", "x", "zh", "co")
    return jax.shard_map(
        local,
        mesh=parts,
        in_specs=(
            P(slab, "zl", None),
            P(None, "zl"),
            P(),
            P(),
            P(),
            P(),
            P(slab, None, "zl"),
            P(slab),
            P(slab),
        ),
        out_specs=(P(slab, None, "zl"), P(slab, None, None), P(None, slab)),
        check_vma=False,
    )
```

```python
import functools
import math

import jax
import jax.numpy as jnp
from jax import lax
from jax.experimental import pallas as pl
from jax.experimental.pallas import tpu as pltpu
from jax.sharding import PartitionSpec as P

LAG = 32
WU = 16
LAGZ = 4
WZ = 4
ROWS = 144


def project_kernel(*refs):
    sources, out, rest = refs[:6], refs[6], refs[7:]
    owner, shift, cls, weights, bank, volume, spreadable, held, mixed, ready, sems = rest
    angles = weights.shape[0]
    columns = volume.shape[1]
    tile = bank.shape[1]
    banks = bank.shape[0]
    tiles = columns // tile
    peers, strips, width = ready.shape
    quarters = peers // angles
    per = tiles // quarters
    coarse = 8
    ring = tiles // coarse
    pair = 2 * tile
    small = [
        pltpu.make_async_copy(source, target, sems.at[i])
        for i, (source, target) in enumerate(zip(sources[:5], rest[:5]))
    ]
    large = []
    for r in range(coarse // 2):
        for j in range(ring):
            where = pl.ds(j * coarse * tile + r * pair, pair)
            large.append(
                pltpu.make_async_copy(
                    sources[5].at[:, where], volume.at[:, where], sems.at[5 + len(large)]
                )
            )
    for copy in small + large:
        copy.start()
    for copy in small:
        copy.wait()
    lane = lax.broadcasted_iota(jnp.int32, (angles, angles), 1)
    wide = jnp.broadcast_to(owner[...].astype(jnp.float32), (angles, angles))
    onehot = (wide.T.astype(jnp.int32) == lane).astype(jnp.float32)
    shifts = jnp.sum(onehot * shift[...].astype(jnp.float32), axis=1, keepdims=True)
    classes = jnp.sum(onehot * cls[...].astype(jnp.float32), axis=1, keepdims=True)
    shifts = jnp.broadcast_to(shifts.astype(jnp.int32), (angles, tile))
    chosen = jnp.dot(
        onehot.astype(jnp.bfloat16), weights[...], preferred_element_type=jnp.float32
    ).astype(jnp.bfloat16)
    classes = jnp.broadcast_to(classes, (angles, tile)).astype(jnp.int32)
    masks = [(classes == c).astype(jnp.bfloat16) for c in range(banks)]
    stacked = bank[...].reshape(banks * tile, tile)
    group = 8
    for r in range(coarse // 2):
        for j in range(ring):
            large[r * ring + j].wait()
            at = j * coarse * tile + r * pair
            ray = jnp.dot(
                chosen, volume[:, at : at + pair], preferred_element_type=jnp.float32
            ).astype(jnp.bfloat16)
            for s in range(2):
                piece = ray[:, s * tile : (s + 1) * tile]
                for c in range(banks):
                    spreadable[
                        s, j * angles : (j + 1) * angles, c * tile : (c + 1) * tile
                    ] = piece * masks[c]
        for s in range(2):
            spread = jnp.dot(spreadable[s], stacked, preferred_element_type=jnp.float32)
            for g in range(angles // group):
                rows = slice(g * group, (g + 1) * group)
                parts = [
                    spread[j * angles + g * group : j * angles + (g + 1) * group]
                    for j in range(ring)
                ]
                for b in range(3):
                    keep = ((shifts[rows] >> (3 + b)) & 1) == 0
                    parts = [
                        jnp.where(keep, parts[j], parts[(j - (1 << b)) % ring])
                        for j in range(ring)
                    ]
                for j in range(ring):
                    at = (j * coarse + 2 * r + s) * tile
                    held[rows, at : at + tile] = parts[j]
    inner = width // tile
    count = angles * strips
    copies = []
    for q in range(quarters):
        for g in range(angles // group):
            rows = slice(g * group, (g + 1) * group)
            parts = []
            for t in range(q * per - coarse + 1, (q + 1) * per):
                at = t % tiles * tile
                parts.append(held[rows, at : at + tile])
            for b in (2, 1, 0):
                step = 1 << b
                keep = ((shifts[rows] >> b) & 1) == 0
                parts = [
                    jnp.where(keep, parts[i], parts[i - step]) for i in range(step, len(parts))
                ]
            for c in range(per):
                p, t = divmod(c, inner)
                at = (q * inner + t) * count + g * group * strips + p
                mixed[pl.ds(at, group, stride=strips), :] = parts[c]
        where = slice(q * angles, (q + 1) * angles)
        for t in range(inner):
            at = (q * inner + t) * count
            block = mixed[at : at + count].astype(jnp.bfloat16)
            ready[where, :, t * tile : (t + 1) * tile] = block.reshape(angles, strips, tile)
        copies.append(pltpu.make_async_copy(ready.at[where], out.at[where], sems.at[q]))
        copies[-1].start()
    for copy in copies:
        copy.wait()


def project(owner, shift, cls, weights, bank, volume, quarters):
    angles = weights.shape[0]
    columns = volume.shape[1]
    tile = bank.shape[1]
    shape = (quarters * angles, 4, columns // quarters // 4)
    small = (owner[None], shift[None], cls[None], weights, bank)
    hbm = pl.BlockSpec(memory_space=pltpu.HBM)
    return pl.pallas_call(
        project_kernel,
        out_shape=jax.ShapeDtypeStruct(shape, jnp.bfloat16),
        in_specs=[hbm] * 6,
        out_specs=hbm,
        scratch_shapes=[pltpu.VMEM(x.shape, x.dtype) for x in small + (volume,)]
        + [
            pltpu.VMEM((2, columns // tile // 8 * angles, bank.shape[0] * tile), jnp.bfloat16),
            pltpu.VMEM((angles, columns), jnp.float32),
            pltpu.VMEM((angles * columns // tile, tile), jnp.float32),
            pltpu.VMEM(shape, jnp.bfloat16),
            pltpu.SemaphoreType.DMA((len(small) + columns // tile // 2,)),
        ],
        name="project",
    )(*small, volume)


def correlate_kernel(norm, starts, parts, across, owned, out, mixed, wide):
    peers, strips, width = parts.shape
    slices, columns = owned.shape
    tile = 128
    tiles = columns // tile
    inner = width // tile
    count = slices * strips
    group = 16
    for g in range(slices // group):
        total = jnp.zeros((group, strips, width), jnp.float32)
        for c in range(peers // slices):
            at = c * slices + g * group
            total = total + parts[at : at + group].astype(jnp.float32)
        for t in range(inner):
            at = t * count + g * group * strips
            block = total[:, :, t * tile : (t + 1) * tile]
            mixed[at : at + group * strips] = block.reshape(group * strips, tile)
    stack = []
    for p in range(strips):
        for t in range(inner):
            block = mixed[pl.ds(t * count + p, slices, stride=strips), :].astype(jnp.bfloat16)
            at = (p * inner + t) * tile
            owned[:, at : at + tile] = block
            stack.append(block)
    rhs = jnp.concatenate(stack, axis=0)
    wide[...] = across[...].astype(jnp.float32)
    start_slice = starts[0]
    first = starts[1] + LAG
    pieces = []
    for a in range(WZ):
        turn = lax.rem(2 * slices - start_slice - a, slices)
        row = []
        for t in range(tiles):
            block = wide[pl.ds(first + t * tile, ROWS), :]
            row.append(pltpu.roll(block, turn, 1).astype(jnp.bfloat16))
        pieces.append(jnp.concatenate(row, axis=1))
    lhs = jnp.concatenate(pieces, axis=0)
    sums = jnp.dot(lhs, rhs, preferred_element_type=jnp.float32)
    lanes = lax.broadcasted_iota(jnp.int32, (8, tile), 1)
    subs = lax.broadcasted_iota(jnp.int32, (8, tile), 0)
    results = []
    for a in range(WZ):
        total = jnp.zeros((8, tile), jnp.float32)
        for i in range(ROWS // 8):
            block = sums[a * ROWS + i * 8 : a * ROWS + i * 8 + 8]
            if i < WU // 8:
                block = jnp.where(lanes < tile // 2, block, 0.0)
            if i >= tile // 8:
                block = jnp.where(lanes >= tile // 2, block, 0.0)
            total = total + pltpu.roll(block, (-8 * i) % tile, 1)
        aligned = jnp.zeros((8, tile), jnp.float32)
        for d in range(WU):
            here = ((subs - d) & (tile - 1)) == lanes
            value = jnp.sum(jnp.where(here, total, 0.0))
            aligned = jnp.where(lanes == d, value, aligned)
        results.append(aligned[0:1])
    results.append(jnp.zeros((8 - WZ, tile), jnp.float32))
    out[...] = jnp.concatenate(results, axis=0) * norm


def correlate(norm, starts, parts, across):
    peers, strips, width = parts.shape
    slices, columns = across.shape[1], strips * width
    vmem = pl.BlockSpec(memory_space=pltpu.VMEM)
    return pl.pallas_call(
        functools.partial(correlate_kernel, norm),
        out_shape=[
            jax.ShapeDtypeStruct((slices, columns), jnp.bfloat16),
            jax.ShapeDtypeStruct((8, 128), jnp.float32),
        ],
        in_specs=[pl.BlockSpec(memory_space=pltpu.SMEM), vmem, vmem],
        scratch_shapes=[
            pltpu.VMEM((slices * columns // 128, 128), jnp.float32),
            pltpu.VMEM(across.shape, jnp.float32),
        ],
        compiler_params=pltpu.CompilerParams(vmem_limit_bytes=14 * 2**20),
        name="correlate",
    )(starts, parts, across)


def finish_kernel(starts, totals, correlation, shifts):
    values = totals[0:WZ, 0:WU]
    correlation[0] = values
    weights = values * values
    lag_slice = starts[0] + lax.broadcasted_iota(jnp.int32, (WZ, WU), 0)
    lag_col = starts[1] + lax.broadcasted_iota(jnp.int32, (WZ, WU), 1)
    count = WZ * WU

    def mean(x):
        return jnp.sum(jnp.sum(x, axis=1, keepdims=True), axis=0, keepdims=True) / count

    denominator = mean(weights) + 1e-06
    by_slice = mean(weights * (lag_slice.astype(jnp.float32) / LAGZ)) / denominator
    by_col = mean(weights * (lag_col.astype(jnp.float32) / LAG)) / denominator
    shifts[...] = jnp.concatenate([by_slice, by_col], axis=1)


def finish(starts, totals):
    return pl.pallas_call(
        finish_kernel,
        out_shape=[
            jax.ShapeDtypeStruct((1, WZ, WU), jnp.float32),
            jax.ShapeDtypeStruct((1, 2), jnp.float32),
        ],
        in_specs=[
            pl.BlockSpec(memory_space=pltpu.SMEM),
            pl.BlockSpec(memory_space=pltpu.VMEM),
        ],
        compiler_params=pltpu.CompilerParams(vmem_limit_bytes=2 * 2**20),
        name="finish",
    )(starts, totals)


def local(
    volume,
    detector_row_weight,
    tile_bank,
    tile_class,
    tile_shift,
    owner_angle,
    measured,
    window_slice,
    window_col,
):
    count = lax.axis_size("zl")
    pieces = project(
        owner_angle, tile_shift, tile_class, detector_row_weight, tile_bank, volume[0], count
    )
    parts = lax.all_to_all(pieces, ("zl", "y", "x", "zh", "co"), 0, 0, tiled=True)
    seen, _ = lax.optimization_barrier((measured[0], pieces))
    slices, quarter = seen.shape
    ring = [(i, (i + 1) % count) for i in range(count)]
    back = [(target, source) for source, target in ring]
    low = lax.ppermute(seen[:, quarter - LAG :], "zl", ring)
    high = lax.ppermute(seen[:, :LAG], "zl", back)
    rest = jnp.zeros((128 - 2 * LAG, slices), jnp.bfloat16)
    across = jnp.concatenate([low.T, seen.T, high.T, rest], axis=0)
    starts = jnp.concatenate([window_slice, window_col])
    norm_factor = 1.0 / math.sqrt(slices * quarter * count)
    owned, part = correlate(norm_factor, starts, parts, across)
    totals, shifts = finish(starts, lax.psum(part, "zl"))
    return (owned[None], totals, shifts.T)


def solution(mesh):
    slab, col = mesh.axis_names
    cols = mesh.shape[col]
    rows = mesh.shape[slab]
    parts = jax.sharding.Mesh(
        mesh.devices.reshape(rows // 16, 4, 2, 2, cols), ("y", "x", "zh", "co", "zl")
    )
    slab = ("y", "x", "zh", "co")
    return jax.shard_map(
        local,
        mesh=parts,
        in_specs=(
            P(slab, "zl", None),
            P(None, "zl"),
            P(),
            P(),
            P(),
            P(),
            P(slab, None, "zl"),
            P(slab),
            P(slab),
        ),
        out_specs=(P(slab, None, "zl"), P(slab, None, None), P(None, slab)),
        check_vma=False,
    )
```

```python
import functools
import math

import jax
import jax.numpy as jnp
from jax import lax
from jax.experimental import pallas as pl
from jax.experimental.pallas import tpu as pltpu
from jax.sharding import PartitionSpec as P

LAG = 32
WU = 16
LAGZ = 4
WZ = 4
ROWS = 144


def project_kernel(*refs):
    sources, out, rest = refs[:6], refs[6], refs[7:]
    owner, shift, cls, weights, bank, volume, held, mixed, ready, sems = rest
    angles = weights.shape[0]
    columns = volume.shape[1]
    tile = bank.shape[1]
    banks = bank.shape[0]
    tiles = columns // tile
    peers, strips, width = ready.shape
    quarters = peers // angles
    per = tiles // quarters
    coarse = 8
    ring = tiles // coarse
    pair = 2 * tile
    small = [
        pltpu.make_async_copy(source, target, sems.at[i])
        for i, (source, target) in enumerate(zip(sources[:5], rest[:5]))
    ]
    large = pltpu.make_async_copy(sources[5], volume, sems.at[5])
    for copy in small + [large]:
        copy.start()
    for copy in small:
        copy.wait()
    lane = lax.broadcasted_iota(jnp.int32, (angles, angles), 1)
    wide = jnp.broadcast_to(owner[...].astype(jnp.float32), (angles, angles))
    onehot = (wide.T.astype(jnp.int32) == lane).astype(jnp.float32)
    shifts = jnp.sum(onehot * shift[...].astype(jnp.float32), axis=1, keepdims=True)
    classes = jnp.sum(onehot * cls[...].astype(jnp.float32), axis=1, keepdims=True)
    shifts = jnp.broadcast_to(shifts.astype(jnp.int32), (angles, tile))
    chosen = jnp.dot(
        onehot.astype(jnp.bfloat16), weights[...], preferred_element_type=jnp.float32
    ).astype(jnp.bfloat16)
    classes = jnp.broadcast_to(classes, (angles, tile)).astype(jnp.int32)
    beside = jnp.concatenate([bank[c] for c in range(banks)], axis=1)
    group = 8
    block = 16
    large.wait()
    for r in range(coarse // 2):
        rays = []
        for j in range(ring):
            at = j * coarse * tile + r * pair
            rays.append(
                jnp.dot(
                    chosen, volume[:, at : at + pair], preferred_element_type=jnp.float32
                ).astype(jnp.bfloat16)
            )
        for s in range(2):
            for first in range(0, angles, 128):
                span = range(first, first + 128, block)
                lhs = jnp.concatenate(
                    [ray[k : k + block, s * tile : (s + 1) * tile] for k in span for ray in rays],
                    axis=0,
                )
                spread = jnp.dot(lhs, beside, preferred_element_type=jnp.float32)
                for i, k in enumerate(span):
                    for half in range(block // group):
                        rows = slice(k + half * group, k + (half + 1) * group)
                        parts = []
                        for j in range(ring):
                            at = (i * ring + j) * block + half * group
                            value = spread[at : at + group]
                            part = value[:, :tile]
                            for c in range(1, banks):
                                part = jnp.where(
                                    classes[rows] == c, value[:, c * tile : (c + 1) * tile], part
                                )
                            parts.append(part)
                        for b in range(3):
                            keep = ((shifts[rows] >> (3 + b)) & 1) == 0
                            parts = [
                                jnp.where(keep, parts[j], parts[(j - (1 << b)) % ring])
                                for j in range(ring)
                            ]
                        for j in range(ring):
                            at = (j * coarse + 2 * r + s) * tile
                            held[rows, at : at + tile] = parts[j]
    inner = width // tile
    count = angles * strips
    copies = []
    for q in range(quarters):
        for g in range(angles // group):
            rows = slice(g * group, (g + 1) * group)
            parts = []
            for t in range(q * per - coarse + 1, (q + 1) * per):
                at = t % tiles * tile
                parts.append(held[rows, at : at + tile])
            for b in (2, 1, 0):
                step = 1 << b
                keep = ((shifts[rows] >> b) & 1) == 0
                parts = [
                    jnp.where(keep, parts[i], parts[i - step]) for i in range(step, len(parts))
                ]
            for c in range(per):
                p, t = divmod(c, inner)
                at = (q * inner + t) * count + g * group * strips + p
                mixed[pl.ds(at, group, stride=strips), :] = parts[c]
        where = slice(q * angles, (q + 1) * angles)
        for t in range(inner):
            at = (q * inner + t) * count
            block = mixed[at : at + count].astype(jnp.bfloat16)
            ready[where, :, t * tile : (t + 1) * tile] = block.reshape(angles, strips, tile)
        copies.append(pltpu.make_async_copy(ready.at[where], out.at[where], sems.at[q]))
        copies[-1].start()
    for copy in copies:
        copy.wait()


def project(owner, shift, cls, weights, bank, volume, quarters):
    angles = weights.shape[0]
    columns = volume.shape[1]
    tile = bank.shape[1]
    shape = (quarters * angles, 4, columns // quarters // 4)
    small = (owner[None], shift[None], cls[None], weights, bank)
    hbm = pl.BlockSpec(memory_space=pltpu.HBM)
    return pl.pallas_call(
        project_kernel,
        out_shape=jax.ShapeDtypeStruct(shape, jnp.bfloat16),
        in_specs=[hbm] * 6,
        out_specs=hbm,
        scratch_shapes=[pltpu.VMEM(x.shape, x.dtype) for x in small + (volume,)]
        + [
            pltpu.VMEM((angles, columns), jnp.float32),
            pltpu.VMEM((angles * columns // tile, tile), jnp.float32),
            pltpu.VMEM(shape, jnp.bfloat16),
            pltpu.SemaphoreType.DMA((len(small) + 1,)),
        ],
        name="project",
    )(*small, volume)


def correlate_kernel(norm, starts, parts, across, owned, out, mixed, wide):
    peers, strips, width = parts.shape
    slices, columns = owned.shape
    tile = 128
    tiles = columns // tile
    inner = width // tile
    count = slices * strips
    group = 16
    for g in range(slices // group):
        total = jnp.zeros((group, strips, width), jnp.float32)
        for c in range(peers // slices):
            at = c * slices + g * group
            total = total + parts[at : at + group].astype(jnp.float32)
        for t in range(inner):
            at = t * count + g * group * strips
            block = total[:, :, t * tile : (t + 1) * tile]
            mixed[at : at + group * strips] = block.reshape(group * strips, tile)
    stack = []
    for p in range(strips):
        for t in range(inner):
            block = mixed[pl.ds(t * count + p, slices, stride=strips), :].astype(jnp.bfloat16)
            at = (p * inner + t) * tile
            owned[:, at : at + tile] = block
            stack.append(block)
    rhs = jnp.concatenate(stack, axis=0)
    wide[...] = across[...].astype(jnp.float32)
    start_slice = starts[0]
    first = starts[1] + LAG
    pieces = []
    for a in range(WZ):
        turn = lax.rem(2 * slices - start_slice - a, slices)
        row = []
        for t in range(tiles):
            block = wide[pl.ds(first + t * tile, ROWS), :]
            row.append(pltpu.roll(block, turn, 1).astype(jnp.bfloat16))
        pieces.append(jnp.concatenate(row, axis=1))
    lhs = jnp.concatenate(pieces, axis=0)
    sums = jnp.dot(lhs, rhs, preferred_element_type=jnp.float32)
    lanes = lax.broadcasted_iota(jnp.int32, (8, tile), 1)
    subs = lax.broadcasted_iota(jnp.int32, (8, tile), 0)
    results = []
    for a in range(WZ):
        total = jnp.zeros((8, tile), jnp.float32)
        for i in range(ROWS // 8):
            block = sums[a * ROWS + i * 8 : a * ROWS + i * 8 + 8]
            if i < WU // 8:
                block = jnp.where(lanes < tile // 2, block, 0.0)
            if i >= tile // 8:
                block = jnp.where(lanes >= tile // 2, block, 0.0)
            total = total + pltpu.roll(block, (-8 * i) % tile, 1)
        aligned = jnp.zeros((8, tile), jnp.float32)
        for d in range(WU):
            here = ((subs - d) & (tile - 1)) == lanes
            value = jnp.sum(jnp.where(here, total, 0.0))
            aligned = jnp.where(lanes == d, value, aligned)
        results.append(aligned[0:1])
    results.append(jnp.zeros((8 - WZ, tile), jnp.float32))
    out[...] = jnp.concatenate(results, axis=0) * norm


def correlate(norm, starts, parts, across):
    peers, strips, width = parts.shape
    slices, columns = across.shape[1], strips * width
    vmem = pl.BlockSpec(memory_space=pltpu.VMEM)
    return pl.pallas_call(
        functools.partial(correlate_kernel, norm),
        out_shape=[
            jax.ShapeDtypeStruct((slices, columns), jnp.bfloat16),
            jax.ShapeDtypeStruct((8, 128), jnp.float32),
        ],
        in_specs=[pl.BlockSpec(memory_space=pltpu.SMEM), vmem, vmem],
        scratch_shapes=[
            pltpu.VMEM((slices * columns // 128, 128), jnp.float32),
            pltpu.VMEM(across.shape, jnp.float32),
        ],
        compiler_params=pltpu.CompilerParams(vmem_limit_bytes=14 * 2**20),
        name="correlate",
    )(starts, parts, across)


def finish_kernel(starts, totals, correlation, shifts):
    values = totals[0:WZ, 0:WU]
    correlation[0] = values
    weights = values * values
    lag_slice = starts[0] + lax.broadcasted_iota(jnp.int32, (WZ, WU), 0)
    lag_col = starts[1] + lax.broadcasted_iota(jnp.int32, (WZ, WU), 1)
    count = WZ * WU

    def mean(x):
        return jnp.sum(jnp.sum(x, axis=1, keepdims=True), axis=0, keepdims=True) / count

    denominator = mean(weights) + 1e-06
    by_slice = mean(weights * (lag_slice.astype(jnp.float32) / LAGZ)) / denominator
    by_col = mean(weights * (lag_col.astype(jnp.float32) / LAG)) / denominator
    shifts[...] = jnp.concatenate([by_slice, by_col], axis=1)


def finish(starts, totals):
    return pl.pallas_call(
        finish_kernel,
        out_shape=[
            jax.ShapeDtypeStruct((1, WZ, WU), jnp.float32),
            jax.ShapeDtypeStruct((1, 2), jnp.float32),
        ],
        in_specs=[
            pl.BlockSpec(memory_space=pltpu.SMEM),
            pl.BlockSpec(memory_space=pltpu.VMEM),
        ],
        compiler_params=pltpu.CompilerParams(vmem_limit_bytes=2 * 2**20),
        name="finish",
    )(starts, totals)


def local(
    volume,
    detector_row_weight,
    tile_bank,
    tile_class,
    tile_shift,
    owner_angle,
    measured,
    window_slice,
    window_col,
):
    count = lax.axis_size("zl")
    pieces = project(
        owner_angle, tile_shift, tile_class, detector_row_weight, tile_bank, volume[0], count
    )
    parts = lax.all_to_all(pieces, ("zl", "y", "x", "zh", "co"), 0, 0, tiled=True)
    seen, _ = lax.optimization_barrier((measured[0], pieces))
    slices, quarter = seen.shape
    ring = [(i, (i + 1) % count) for i in range(count)]
    back = [(target, source) for source, target in ring]
    low = lax.ppermute(seen[:, quarter - LAG :], "zl", ring)
    high = lax.ppermute(seen[:, :LAG], "zl", back)
    rest = jnp.zeros((128 - 2 * LAG, slices), jnp.bfloat16)
    across = jnp.concatenate([low.T, seen.T, high.T, rest], axis=0)
    starts = jnp.concatenate([window_slice, window_col])
    norm_factor = 1.0 / math.sqrt(slices * quarter * count)
    owned, part = correlate(norm_factor, starts, parts, across)
    totals, shifts = finish(starts, lax.psum(part, "zl"))
    return (owned[None], totals, shifts.T)


def solution(mesh):
    slab, col = mesh.axis_names
    cols = mesh.shape[col]
    rows = mesh.shape[slab]
    parts = jax.sharding.Mesh(
        mesh.devices.reshape(rows // 16, 4, 2, 2, cols), ("y", "x", "zh", "co", "zl")
    )
    slab = ("y", "x", "zh", "co")
    return jax.shard_map(
        local,
        mesh=parts,
        in_specs=(
            P(slab, "zl", None),
            P(None, "zl"),
            P(),
            P(),
            P(),
            P(),
            P(slab, None, "zl"),
            P(slab),
            P(slab),
        ),
        out_specs=(P(slab, None, "zl"), P(slab, None, None), P(None, slab)),
        check_vma=False,
    )
```

```python
import functools
import math

import jax
import jax.numpy as jnp
from jax import lax
from jax.experimental import pallas as pl
from jax.experimental.pallas import tpu as pltpu
from jax.sharding import PartitionSpec as P

LAG = 32
WU = 16
LAGZ = 4
WZ = 4
ROWS = 144
EVERY = ("zl", "y", "x", "zh", "co")


def project_kernel(quarters, *refs):
    sources, out, rest = refs[:6], refs[6], refs[7:]
    owner, shift, cls, weights, bank, volume, held, mixed, ready, sems = rest
    angles = weights.shape[0]
    columns = volume.shape[1]
    tile = bank.shape[1]
    banks = bank.shape[0]
    tiles = columns // tile
    per = tiles // quarters
    coarse = 8
    ring = tiles // coarse
    pair = 2 * tile
    small = [
        pltpu.make_async_copy(source, target, sems.at[i])
        for i, (source, target) in enumerate(zip(sources[:5], rest[:5]))
    ]
    large = pltpu.make_async_copy(sources[5], volume, sems.at[5])
    for copy in small + [large]:
        copy.start()
    for copy in small:
        copy.wait()
    lane = lax.broadcasted_iota(jnp.int32, (angles, angles), 1)
    wide = jnp.broadcast_to(owner[...].astype(jnp.float32), (angles, angles))
    onehot = (wide.T.astype(jnp.int32) == lane).astype(jnp.float32)
    shifts = jnp.sum(onehot * shift[...].astype(jnp.float32), axis=1, keepdims=True)
    classes = jnp.sum(onehot * cls[...].astype(jnp.float32), axis=1, keepdims=True)
    shifts = jnp.broadcast_to(shifts.astype(jnp.int32), (angles, tile))
    chosen = jnp.dot(
        onehot.astype(jnp.bfloat16), weights[...], preferred_element_type=jnp.float32
    ).astype(jnp.bfloat16)
    classes = jnp.broadcast_to(classes, (angles, tile)).astype(jnp.int32)
    beside = jnp.concatenate([bank[c] for c in range(banks)], axis=1)
    group = 8
    block = 16
    large.wait()
    for r in range(coarse // 2):
        rays = []
        for j in range(ring):
            at = j * coarse * tile + r * pair
            rays.append(
                jnp.dot(
                    chosen, volume[:, at : at + pair], preferred_element_type=jnp.float32
                ).astype(jnp.bfloat16)
            )
        for s in range(2):
            for first in range(0, angles, 128):
                span = range(first, first + 128, block)
                lhs = jnp.concatenate(
                    [ray[k : k + block, s * tile : (s + 1) * tile] for k in span for ray in rays],
                    axis=0,
                )
                spread = jnp.dot(lhs, beside, preferred_element_type=jnp.float32)
                for i, k in enumerate(span):
                    for half in range(block // group):
                        rows = slice(k + half * group, k + (half + 1) * group)
                        parts = []
                        for j in range(ring):
                            at = (i * ring + j) * block + half * group
                            value = spread[at : at + group]
                            part = value[:, :tile]
                            for c in range(1, banks):
                                part = jnp.where(
                                    classes[rows] == c, value[:, c * tile : (c + 1) * tile], part
                                )
                            parts.append(part)
                        for b in range(3):
                            keep = ((shifts[rows] >> (3 + b)) & 1) == 0
                            parts = [
                                jnp.where(keep, parts[j], parts[(j - (1 << b)) % ring])
                                for j in range(ring)
                            ]
                        for j in range(ring):
                            at = (j * coarse + 2 * r + s) * tile
                            held[rows, at : at + tile] = parts[j]
    count = angles * per
    copies = []
    for q in range(quarters):
        for g in range(angles // group):
            rows = slice(g * group, (g + 1) * group)
            parts = []
            for t in range(q * per - coarse + 1, (q + 1) * per):
                at = t % tiles * tile
                parts.append(held[rows, at : at + tile])
            for b in (2, 1, 0):
                step = 1 << b
                keep = ((shifts[rows] >> b) & 1) == 0
                parts = [
                    jnp.where(keep, parts[i], parts[i - step]) for i in range(step, len(parts))
                ]
            for c in range(per):
                mixed[pl.ds(q * count + g * group * per + c, group, stride=per), :] = parts[c]
        where = slice(q * count, (q + 1) * count)
        ready[where] = mixed[where].astype(jnp.bfloat16)
        copies.append(pltpu.make_async_copy(ready.at[where], out.at[where], sems.at[q]))
        copies[-1].start()
    for copy in copies:
        copy.wait()


def project(owner, shift, cls, weights, bank, volume, quarters):
    angles = weights.shape[0]
    columns = volume.shape[1]
    tile = bank.shape[1]
    shape = (angles * columns // tile, tile)
    small = (owner[None], shift[None], cls[None], weights, bank)
    hbm = pl.BlockSpec(memory_space=pltpu.HBM)
    return pl.pallas_call(
        functools.partial(project_kernel, quarters),
        out_shape=jax.ShapeDtypeStruct(shape, jnp.bfloat16),
        in_specs=[hbm] * 6,
        out_specs=hbm,
        scratch_shapes=[pltpu.VMEM(x.shape, x.dtype) for x in small + (volume,)]
        + [
            pltpu.VMEM((angles, columns), jnp.float32),
            pltpu.VMEM(shape, jnp.float32),
            pltpu.VMEM(shape, jnp.bfloat16),
            pltpu.SemaphoreType.DMA((len(small) + 1,)),
        ],
        name="project",
    )(*small, volume)


def correlate_kernel(norm, starts, parts, across, owned, out, mixed, wide):
    slices, columns = owned.shape
    tile = parts.shape[1]
    tiles = columns // tile
    count = slices * tiles
    group = 64
    for at in range(0, count, group):
        total = parts[at : at + group].astype(jnp.float32)
        for c in range(1, parts.shape[0] // count):
            block = parts[c * count + at : c * count + at + group]
            total = total + block.astype(jnp.float32)
        mixed[at : at + group] = total
    stack = []
    for t in range(tiles):
        block = mixed[pl.ds(t, slices, stride=tiles), :].astype(jnp.bfloat16)
        owned[:, t * tile : (t + 1) * tile] = block
        stack.append(block)
    rhs = jnp.concatenate(stack, axis=0)
    wide[...] = across[...].astype(jnp.float32)
    start_slice = starts[0]
    first = starts[1] + LAG
    pieces = []
    for a in range(WZ):
        turn = lax.rem(2 * slices - start_slice - a, slices)
        row = []
        for t in range(tiles):
            block = wide[pl.ds(first + t * tile, ROWS), :]
            row.append(pltpu.roll(block, turn, 1).astype(jnp.bfloat16))
        pieces.append(jnp.concatenate(row, axis=1))
    lhs = jnp.concatenate(pieces, axis=0)
    sums = jnp.dot(lhs, rhs, preferred_element_type=jnp.float32)
    lanes = lax.broadcasted_iota(jnp.int32, (8, tile), 1)
    subs = lax.broadcasted_iota(jnp.int32, (8, tile), 0)
    results = []
    for a in range(WZ):
        total = jnp.zeros((8, tile), jnp.float32)
        for i in range(ROWS // 8):
            block = sums[a * ROWS + i * 8 : a * ROWS + i * 8 + 8]
            if i < WU // 8:
                block = jnp.where(lanes < tile // 2, block, 0.0)
            if i >= tile // 8:
                block = jnp.where(lanes >= tile // 2, block, 0.0)
            total = total + pltpu.roll(block, (-8 * i) % tile, 1)
        aligned = jnp.zeros((8, tile), jnp.float32)
        for d in range(WU):
            here = ((subs - d) & (tile - 1)) == lanes
            value = jnp.sum(jnp.where(here, total, 0.0))
            aligned = jnp.where(lanes == d, value, aligned)
        results.append(aligned[0:1])
    results.append(jnp.zeros((8 - WZ, tile), jnp.float32))
    out[...] = jnp.concatenate(results, axis=0) * norm


def correlate(norm, starts, parts, across, count):
    slices = across.shape[1]
    columns = parts.size // slices // count
    vmem = pl.BlockSpec(memory_space=pltpu.VMEM)
    return pl.pallas_call(
        functools.partial(correlate_kernel, norm),
        out_shape=[
            jax.ShapeDtypeStruct((slices, columns), jnp.bfloat16),
            jax.ShapeDtypeStruct((8, 128), jnp.float32),
        ],
        in_specs=[pl.BlockSpec(memory_space=pltpu.SMEM), vmem, vmem],
        scratch_shapes=[
            pltpu.VMEM((slices * columns // 128, 128), jnp.float32),
            pltpu.VMEM(across.shape, jnp.float32),
        ],
        compiler_params=pltpu.CompilerParams(vmem_limit_bytes=14 * 2**20),
        name="correlate",
    )(starts, parts, across)


def finish_kernel(starts, totals, correlation, shifts):
    values = totals[0:WZ, 0:WU]
    correlation[0] = values
    weights = values * values
    lag_slice = starts[0] + lax.broadcasted_iota(jnp.int32, (WZ, WU), 0)
    lag_col = starts[1] + lax.broadcasted_iota(jnp.int32, (WZ, WU), 1)
    count = WZ * WU

    def mean(x):
        return jnp.sum(jnp.sum(x, axis=1, keepdims=True), axis=0, keepdims=True) / count

    denominator = mean(weights) + 1e-06
    by_slice = mean(weights * (lag_slice.astype(jnp.float32) / LAGZ)) / denominator
    by_col = mean(weights * (lag_col.astype(jnp.float32) / LAG)) / denominator
    shifts[...] = jnp.concatenate([by_slice, by_col], axis=1)


def finish(starts, totals):
    return pl.pallas_call(
        finish_kernel,
        out_shape=[
            jax.ShapeDtypeStruct((1, WZ, WU), jnp.float32),
            jax.ShapeDtypeStruct((1, 2), jnp.float32),
        ],
        in_specs=[
            pl.BlockSpec(memory_space=pltpu.SMEM),
            pl.BlockSpec(memory_space=pltpu.VMEM),
        ],
        compiler_params=pltpu.CompilerParams(vmem_limit_bytes=2 * 2**20),
        name="finish",
    )(starts, totals)


def local(
    volume,
    detector_row_weight,
    tile_bank,
    tile_class,
    tile_shift,
    owner_angle,
    measured,
    window_slice,
    window_col,
):
    count = lax.axis_size("zl")
    pieces = project(
        owner_angle, tile_shift, tile_class, detector_row_weight, tile_bank, volume[0], count
    )
    peers = math.prod(lax.axis_size(axis) for axis in EVERY)
    parts = lax.all_to_all(
        pieces.reshape(-1, 4, 128).reshape(peers, -1, 4, 128), EVERY, 0, 0, tiled=True
    ).reshape(-1, 4, 128).reshape(pieces.shape)
    seen, _ = lax.optimization_barrier((measured[0], pieces))
    slices, quarter = seen.shape
    ring = [(i, (i + 1) % count) for i in range(count)]
    back = [(target, source) for source, target in ring]
    low = lax.ppermute(seen[:, quarter - LAG :], "zl", ring)
    high = lax.ppermute(seen[:, :LAG], "zl", back)
    rest = jnp.zeros((128 - 2 * LAG, slices), jnp.bfloat16)
    across = jnp.concatenate([low.T, seen.T, high.T, rest], axis=0)
    starts = jnp.concatenate([window_slice, window_col])
    norm_factor = 1.0 / math.sqrt(slices * quarter * count)
    owned, part = correlate(norm_factor, starts, parts, across, count)
    totals, shifts = finish(starts, lax.psum(part, "zl"))
    return (owned[None], totals, shifts.T)


def solution(mesh):
    slab, col = mesh.axis_names
    cols = mesh.shape[col]
    rows = mesh.shape[slab]
    parts = jax.sharding.Mesh(
        mesh.devices.reshape(rows // 16, 4, 2, 2, cols), ("y", "x", "zh", "co", "zl")
    )
    slab = ("y", "x", "zh", "co")
    return jax.shard_map(
        local,
        mesh=parts,
        in_specs=(
            P(slab, "zl", None),
            P(None, "zl"),
            P(),
            P(),
            P(),
            P(),
            P(slab, None, "zl"),
            P(slab),
            P(slab),
        ),
        out_specs=(P(slab, None, "zl"), P(slab, None, None), P(None, slab)),
        check_vma=False,
    )
```

```python
import functools
import math

import jax
import jax.numpy as jnp
from jax import lax
from jax.experimental import pallas as pl
from jax.experimental.pallas import tpu as pltpu
from jax.sharding import PartitionSpec as P

LAG = 32
WU = 16
LAGZ = 4
WZ = 4
ROWS = 144
EVERY = ("zl", "y", "x", "zh", "co")


def project_kernel(quarters, *refs):
    sources, out, rest = refs[:6], refs[6], refs[7:]
    owner, shift, cls, weights, bank, volume, held, mixed, ready, sems = rest
    angles = weights.shape[0]
    columns = volume.shape[1]
    tile = bank.shape[1]
    banks = bank.shape[0]
    tiles = columns // tile
    per = tiles // quarters
    coarse = 8
    ring = tiles // coarse
    pair = 2 * tile
    small = [
        pltpu.make_async_copy(source, target, sems.at[i])
        for i, (source, target) in enumerate(zip(sources[:5], rest[:5]))
    ]
    large = pltpu.make_async_copy(sources[5], volume, sems.at[5])
    for copy in small + [large]:
        copy.start()
    for copy in small:
        copy.wait()
    lane = lax.broadcasted_iota(jnp.int32, (angles, angles), 1)
    wide = jnp.broadcast_to(owner[...].astype(jnp.float32), (angles, angles))
    onehot = (wide.T.astype(jnp.int32) == lane).astype(jnp.float32)
    shifts = jnp.sum(onehot * shift[...].astype(jnp.float32), axis=1, keepdims=True)
    classes = jnp.sum(onehot * cls[...].astype(jnp.float32), axis=1, keepdims=True)
    shifts = jnp.broadcast_to(shifts.astype(jnp.int32), (angles, tile))
    chosen = jnp.dot(
        onehot.astype(jnp.bfloat16), weights[...], preferred_element_type=jnp.float32
    ).astype(jnp.bfloat16)
    classes = jnp.broadcast_to(classes, (angles, tile)).astype(jnp.int32)
    beside = jnp.concatenate([bank[c] for c in range(banks)], axis=1)
    group = 8
    block = 16
    large.wait()
    for r in range(coarse // 2):
        rays = []
        for j in range(ring):
            at = j * coarse * tile + r * pair
            rays.append(
                jnp.dot(
                    chosen, volume[:, at : at + pair], preferred_element_type=jnp.float32
                ).astype(jnp.bfloat16)
            )
        for s in range(2):
            for first in range(0, angles, 128):
                span = range(first, first + 128, block)
                lhs = jnp.concatenate(
                    [ray[k : k + block, s * tile : (s + 1) * tile] for k in span for ray in rays],
                    axis=0,
                )
                spread = jnp.dot(lhs, beside, preferred_element_type=jnp.float32)
                for i, k in enumerate(span):
                    for half in range(block // group):
                        rows = slice(k + half * group, k + (half + 1) * group)
                        parts = []
                        for j in range(ring):
                            at = (i * ring + j) * block + half * group
                            value = spread[at : at + group]
                            part = value[:, :tile]
                            for c in range(1, banks):
                                part = jnp.where(
                                    classes[rows] == c, value[:, c * tile : (c + 1) * tile], part
                                )
                            parts.append(part)
                        for b in range(3):
                            keep = ((shifts[rows] >> (3 + b)) & 1) == 0
                            parts = [
                                jnp.where(keep, parts[j], parts[(j - (1 << b)) % ring])
                                for j in range(ring)
                            ]
                        for j in range(ring):
                            at = (j * coarse + 2 * r + s) * tile
                            held[rows, at : at + tile] = parts[j]
    count = angles * per
    copies = []
    for q in range(quarters):
        for g in range(angles // group):
            rows = slice(g * group, (g + 1) * group)
            parts = []
            for t in range(q * per - coarse + 1, (q + 1) * per):
                at = t % tiles * tile
                parts.append(held[rows, at : at + tile])
            for b in (2, 1, 0):
                step = 1 << b
                keep = ((shifts[rows] >> b) & 1) == 0
                parts = [
                    jnp.where(keep, parts[i], parts[i - step]) for i in range(step, len(parts))
                ]
            for c in range(per):
                mixed[pl.ds(q * count + g * group * per + c, group, stride=per), :] = parts[c]
        where = slice(q * count, (q + 1) * count)
        ready[where] = mixed[where].astype(jnp.bfloat16)
        copies.append(pltpu.make_async_copy(ready.at[where], out.at[where], sems.at[q]))
        copies[-1].start()
    for copy in copies:
        copy.wait()


def project(owner, shift, cls, weights, bank, volume, quarters):
    angles = weights.shape[0]
    columns = volume.shape[1]
    tile = bank.shape[1]
    shape = (angles * columns // tile, tile)
    small = (owner[None], shift[None], cls[None], weights, bank)
    hbm = pl.BlockSpec(memory_space=pltpu.HBM)
    return pl.pallas_call(
        functools.partial(project_kernel, quarters),
        out_shape=jax.ShapeDtypeStruct(shape, jnp.bfloat16),
        in_specs=[hbm] * 6,
        out_specs=hbm,
        scratch_shapes=[pltpu.VMEM(x.shape, x.dtype) for x in small + (volume,)]
        + [
            pltpu.VMEM((angles, columns), jnp.float32),
            pltpu.VMEM(shape, jnp.float32),
            pltpu.VMEM(shape, jnp.bfloat16),
            pltpu.SemaphoreType.DMA((len(small) + 1,)),
        ],
        name="project",
    )(*small, volume)


def align_kernel(starts, across, lhs, wide):
    slices = across.shape[1]
    tiles = lhs.shape[1] // slices
    wide[...] = across[...].astype(jnp.float32)
    first = starts[1] + LAG
    for a in range(WZ):
        turn = lax.rem(2 * slices - starts[0] - a, slices)
        for t in range(tiles):
            block = wide[pl.ds(first + t * slices, ROWS), :]
            lhs[a * ROWS : (a + 1) * ROWS, t * slices : (t + 1) * slices] = pltpu.roll(
                block, turn, 1
            ).astype(jnp.bfloat16)


def align(starts, across, tiles):
    vmem = pl.BlockSpec(memory_space=pltpu.VMEM)
    return pl.pallas_call(
        align_kernel,
        out_shape=jax.ShapeDtypeStruct((WZ * ROWS, tiles * across.shape[1]), jnp.bfloat16),
        in_specs=[pl.BlockSpec(memory_space=pltpu.SMEM), vmem],
        scratch_shapes=[pltpu.VMEM(across.shape, jnp.float32)],
        compiler_params=pltpu.CompilerParams(vmem_limit_bytes=8 * 2**20),
        name="align",
    )(starts, across)


def correlate_kernel(norm, parts, lhs, owned, out, mixed, ready, sem):
    slices, columns = owned.shape
    tile = parts.shape[1]
    tiles = columns // tile
    count = slices * tiles
    group = 64
    for at in range(0, count, group):
        total = parts[at : at + group].astype(jnp.float32)
        for c in range(1, parts.shape[0] // count):
            block = parts[c * count + at : c * count + at + group]
            total = total + block.astype(jnp.float32)
        mixed[at : at + group] = total
    stack = []
    for t in range(tiles):
        block = mixed[pl.ds(t, slices, stride=tiles), :].astype(jnp.bfloat16)
        ready[:, t * tile : (t + 1) * tile] = block
        stack.append(block)
    copy = pltpu.make_async_copy(ready, owned, sem.at[0])
    copy.start()
    rhs = jnp.concatenate(stack, axis=0)
    sums = jnp.dot(lhs[...], rhs, preferred_element_type=jnp.float32)
    lanes = lax.broadcasted_iota(jnp.int32, (8, tile), 1)
    subs = lax.broadcasted_iota(jnp.int32, (8, tile), 0)
    results = []
    for a in range(WZ):
        total = jnp.zeros((8, tile), jnp.float32)
        for i in range(ROWS // 8):
            block = sums[a * ROWS + i * 8 : a * ROWS + i * 8 + 8]
            if i < WU // 8:
                block = jnp.where(lanes < tile // 2, block, 0.0)
            if i >= tile // 8:
                block = jnp.where(lanes >= tile // 2, block, 0.0)
            total = total + pltpu.roll(block, (-8 * i) % tile, 1)
        aligned = jnp.zeros((8, tile), jnp.float32)
        for d in range(WU):
            here = ((subs - d) & (tile - 1)) == lanes
            value = jnp.sum(jnp.where(here, total, 0.0))
            aligned = jnp.where(lanes == d, value, aligned)
        results.append(aligned[0:1])
    results.append(jnp.zeros((8 - WZ, tile), jnp.float32))
    values = jnp.concatenate(results, axis=0) * norm
    for peer in range(out.shape[0]):
        out[peer] = values
    copy.wait()


def correlate(norm, parts, lhs, count):
    slices = parts.size // count // lhs.shape[1]
    vmem = pl.BlockSpec(memory_space=pltpu.VMEM)
    return pl.pallas_call(
        functools.partial(correlate_kernel, norm),
        out_shape=[
            jax.ShapeDtypeStruct((slices, lhs.shape[1]), jnp.bfloat16),
            jax.ShapeDtypeStruct((count, 8, 128), jnp.float32),
        ],
        in_specs=[vmem, vmem],
        out_specs=[pl.BlockSpec(memory_space=pltpu.HBM), vmem],
        scratch_shapes=[
            pltpu.VMEM((parts.shape[0] // count, parts.shape[1]), jnp.float32),
            pltpu.VMEM((slices, lhs.shape[1]), jnp.bfloat16),
            pltpu.SemaphoreType.DMA((1,)),
        ],
        compiler_params=pltpu.CompilerParams(vmem_limit_bytes=14 * 2**20),
        name="correlate",
    )(parts, lhs)


def finish_kernel(starts, totals, correlation, shifts):
    values = totals[0, 0:WZ, 0:WU]
    for c in range(1, totals.shape[0]):
        values = values + totals[c, 0:WZ, 0:WU]
    correlation[0] = values
    weights = values * values
    lag_slice = starts[0] + lax.broadcasted_iota(jnp.int32, (WZ, WU), 0)
    lag_col = starts[1] + lax.broadcasted_iota(jnp.int32, (WZ, WU), 1)
    count = WZ * WU

    def mean(x):
        return jnp.sum(jnp.sum(x, axis=1, keepdims=True), axis=0, keepdims=True) / count

    denominator = mean(weights) + 1e-06
    by_slice = mean(weights * (lag_slice.astype(jnp.float32) / LAGZ)) / denominator
    by_col = mean(weights * (lag_col.astype(jnp.float32) / LAG)) / denominator
    shifts[...] = jnp.concatenate([by_slice, by_col], axis=1)


def finish(starts, totals):
    return pl.pallas_call(
        finish_kernel,
        out_shape=[
            jax.ShapeDtypeStruct((1, WZ, WU), jnp.float32),
            jax.ShapeDtypeStruct((1, 2), jnp.float32),
        ],
        in_specs=[
            pl.BlockSpec(memory_space=pltpu.SMEM),
            pl.BlockSpec(memory_space=pltpu.VMEM),
        ],
        compiler_params=pltpu.CompilerParams(vmem_limit_bytes=2 * 2**20),
        name="finish",
    )(starts, totals)


def local(
    volume,
    detector_row_weight,
    tile_bank,
    tile_class,
    tile_shift,
    owner_angle,
    measured,
    window_slice,
    window_col,
):
    count = lax.axis_size("zl")
    pieces = project(
        owner_angle, tile_shift, tile_class, detector_row_weight, tile_bank, volume[0], count
    )
    peers = math.prod(lax.axis_size(axis) for axis in EVERY)
    parts = lax.all_to_all(
        pieces.reshape(-1, 4, 128).reshape(peers, -1, 4, 128), EVERY, 0, 0, tiled=True
    ).reshape(-1, 4, 128).reshape(pieces.shape)
    seen, _ = lax.optimization_barrier((measured[0], pieces))
    slices, quarter = seen.shape
    ring = [(i, (i + 1) % count) for i in range(count)]
    back = [(target, source) for source, target in ring]
    low = lax.ppermute(seen[:, quarter - LAG :], "zl", ring)
    high = lax.ppermute(seen[:, :LAG], "zl", back)
    rest = jnp.zeros((128 - 2 * LAG, slices), jnp.bfloat16)
    across = jnp.concatenate([low.T, seen.T, high.T, rest], axis=0)
    starts = jnp.concatenate([window_slice, window_col])
    norm_factor = 1.0 / math.sqrt(slices * quarter * count)
    lhs = align(starts, across, quarter // slices)
    owned, part = correlate(norm_factor, parts, lhs, count)
    shares = lax.all_to_all(part, "zl", 0, 0, tiled=True)
    totals, shifts = finish(starts, shares)
    return (owned[None], totals, shifts.T)


def solution(mesh):
    slab, col = mesh.axis_names
    cols = mesh.shape[col]
    rows = mesh.shape[slab]
    parts = jax.sharding.Mesh(
        mesh.devices.reshape(rows // 16, 4, 2, 2, cols), ("y", "x", "zh", "co", "zl")
    )
    slab = ("y", "x", "zh", "co")
    return jax.shard_map(
        local,
        mesh=parts,
        in_specs=(
            P(slab, "zl", None),
            P(None, "zl"),
            P(),
            P(),
            P(),
            P(),
            P(slab, None, "zl"),
            P(slab),
            P(slab),
        ),
        out_specs=(P(slab, None, "zl"), P(slab, None, None), P(None, slab)),
        check_vma=False,
    )
```
